32 devices in a mesh: gr: 8 (over z, core), gc: 4 (over y, x).
Axes of the slice: x: 2, y: 2, z: 4, core: 2. Of those that a mesh axis runs over, the one named last changes fastest.
Arguments:
- projectors: bfloat16 [2, 8192, 9216], P(None, ('gr', 'gc')), may hold values from -0.0625 to 0.0625
- wavefunctions: bfloat16 [2, 8192, 512], P(None, ('gr', 'gc')), may hold values from -6 to 6
- coupling: float32 [512, 18, 18], P('gc'), may hold values from -1.5 to 1.5
- atom_order: int32 [512], replicated, may hold values from 0 to 511, each once
Outputs:
- coupled: float32 [9216, 512], P('gc', 'gr')
The draws below stay inside these ranges and needn't reach their ends.
Inputs may be any that keep to these rules, and one draw needn't show every extreme that they name: `atom_order`: a permutation of the atoms.
All inputs are finite; a program needn't handle non-finite values.
Results may differ from the reference program's by a relative error of at most 0.0003.
Values sent between devices are 32-bit elements; how exact they have to be, the bound alone decides.
No kernel may reach another device: no remote copies, remote signals or barrier semaphores. Data moves between devices by JAX's collectives and lax.ppermute only.
A program may use at most 128 MiB of HBM per device.

```python
import jax
import jax.numpy as jnp
from jax import lax

ATOMS = 512
NH = 18
BANDS = 512
NKB = 9216
NPW = 8192


def spiked(drawn, key, source, target, parts, factor):
    def block_of(position):
        return (jnp.arange(drawn.shape[position]) // (drawn.shape[position] // parts)).reshape((-1,) + (1,) * (drawn.ndim - 1 - position))

    first = jax.random.permutation(key, parts)[block_of(target)]
    second = (block_of(target) + parts // 2) % parts
    return jnp.where((block_of(source) == first) | (block_of(source) == second), factor * drawn, drawn)


def block_scale(own_key, extent, cuts, least, largest):
    level, own = 1.0, jax.random.fold_in(own_key, 6)
    for dim, blocks in cuts:
        heights = jnp.exp(jax.random.uniform(jax.random.fold_in(own, dim), (blocks,), jnp.float32, least / len(cuts), largest / len(cuts)))
        level = level * jnp.repeat(heights, extent[dim] // blocks).reshape([-1 if axis == dim else 1 for axis in range(len(extent))])
    return level


def scatter_about(own_key, shape, width, reach, split=(), dtype=jnp.bfloat16):
    drawn = jax.random.normal(own_key, shape, jnp.float32) * width
    if len(split) > 0:
        drawn = block_scale(own_key, shape, split, -0.22, 0.18) * drawn
    return jnp.clip(drawn, min=-reach, max=reach).astype(dtype)


def heavy_noise(key, extent, width, reach, split, heavy, dtype=jnp.bfloat16):
    drawn = width * jax.random.normal(key, extent, jnp.float32)
    if split:
        drawn = drawn * block_scale(key, extent, split, -0.22, 0.18)
    return jnp.clip(spiked(drawn, jax.random.fold_in(key, 3), *heavy), -reach, reach).astype(dtype)


def setup_inputs(seed: int = 0) -> dict:
    seeds = jax.random.split(jax.random.key(seed), 5)
    return {
        "projectors": heavy_noise(seeds[0], (2, NPW, NKB), (4 * NPW) ** -0.5, 0.0625, ((1, 32),), (1, 2, 32, 2.75)),
        "wavefunctions": scatter_about(seeds[1], (2, NPW, BANDS), 1.0, 6.0, ((1, 32),)),
        "coupling": scatter_about(seeds[2], (ATOMS, NH, NH), NH ** -0.5, 1.5, ((0, 4),), jnp.float32),
        "atom_order": jax.random.permutation(seeds[3], ATOMS).astype(jnp.int32),
    }


def reference(projectors, wavefunctions, coupling, atom_order):
    shaped = projectors.reshape(2, NPW, ATOMS, NH)
    waves = wavefunctions.reshape(2 * NPW, BANDS)
    blocks = atom_order.reshape(-1, 32)

    def one_block(picked_ids):
        columns = jnp.take(shaped, picked_ids, axis=2).reshape(2 * NPW, 32 * NH)
        term = lax.dot_general(columns, waves, (((0,), (0,)), ((), ())), preferred_element_type=jnp.float32)
        return 2.0 * term

    becp = lax.map(one_block, blocks).reshape(ATOMS, NH, BANDS)
    coupled = jnp.einsum("kij,kjb->kib", coupling.astype(jnp.float32), becp, precision=lax.Precision.HIGHEST)
    return coupled.reshape(NKB, BANDS)
```

```python
import functools

import jax
import jax.numpy as jnp
from jax import lax
from jax.experimental import pallas as pl
from jax.experimental.pallas import tpu as pltpu
from jax.sharding import PartitionSpec as P

CALLS = 2
PER_CALL = 2
GROUP = 4
PAD = 8
LANES = 128


def project_body(atoms_ref, proj_ref, waves_ref, *rest, steps, owners, nh, per_block, width):
    outs, nat_ref = rest[:-1], rest[-1]
    step = pl.program_id(0)
    block = proj_ref.shape[1]

    @pl.when(step < steps)
    def _():
        start = pl.multiple_of(PAD + step * block, 8)
        term = lax.dot_general(
            proj_ref[...], waves_ref[...], (((0,), (0,)), ((), ())), preferred_element_type=jnp.float32
        )
        for lane in range(term.shape[1] // LANES):
            nat_ref[lane, pl.ds(start, block), :] = term[:, lane * LANES:(lane + 1) * LANES]

    tiles = GROUP * nh // 8
    for chunk in range(len(outs) // 2):
        keep_ref, send_ref = outs[2 * chunk], outs[2 * chunk + 1]
        first = steps + chunk * owners

        @pl.when((step >= first) & (step < first + owners))
        def _():
            @pl.loop(0, per_block // GROUP)
            def _(g):
                slot = (step - steps) * per_block + g * GROUP
                starts = [atoms_ref[slot + t] * nh + PAD for t in range(GROUP)]
                for tile in range(tiles):
                    row = tile * 8
                    a = row // nh
                    at = pl.multiple_of(g * (GROUP * nh) + row, 8)
                    for lane in range(2 * width // LANES):
                        vals = nat_ref[lane, pl.ds(starts[a] + (row - a * nh), 8), :]
                        if (row + 7) // nh != a:
                            cut = (a + 1) * nh - row
                            nxt = nat_ref[lane, pl.ds(starts[a + 1] - cut, 8), :]
                            sub = lax.broadcasted_iota(jnp.int32, vals.shape, 0)
                            vals = jnp.where(sub < cut, vals, nxt)
                        out_ref = keep_ref if lane * LANES < width else send_ref
                        out_ref[pl.ds(at, 8), pl.ds(lane * LANES % width, LANES)] = vals


def project(columns, waves, atoms, owners, nh, per_block):
    k, nkb = columns.shape
    bands = waves.shape[1]
    width = bands // 2
    block = nkb // 8
    steps = nkb // block
    chunks = atoms.shape[0] // (owners * per_block)
    rows = per_block * nh

    def out_map(chunk):
        return lambda i, *_: (jnp.clip(i - steps - chunk * owners, 0, owners - 1), 0)

    specs, shapes = [], []
    for chunk in range(chunks):
        for _ in range(2):
            specs.append(pl.BlockSpec((rows, width), out_map(chunk)))
            shapes.append(jax.ShapeDtypeStruct((owners * rows, width), jnp.float32))
    body = functools.partial(project_body, steps=steps, owners=owners, nh=nh, per_block=per_block, width=width)
    return pl.pallas_call(
        body,
        grid_spec=pltpu.PrefetchScalarGridSpec(
            num_scalar_prefetch=1,
            grid=(steps + chunks * owners,),
            in_specs=[
                pl.BlockSpec((k, block), lambda i, *_: (0, jnp.minimum(i, steps - 1))),
                pl.BlockSpec((k, bands), lambda i, *_: (0, 0)),
            ],
            out_specs=specs,
            scratch_shapes=[pltpu.VMEM((bands // LANES, nkb + 2 * PAD, LANES), jnp.float32)],
        ),
        out_shape=shapes,
        compiler_params=pltpu.CompilerParams(
            dimension_semantics=("arbitrary",), vmem_limit_bytes=48 * 1024 * 1024
        ),
        cost_estimate=pl.CostEstimate(
            flops=2 * k * nkb * bands, transcendentals=0, bytes_accessed=2 * k * nkb + 4 * nkb * bands
        ),
    )(atoms, columns, waves)


def swap(x, axis, bit):
    n = lax.axis_size(axis)
    return lax.ppermute(x, axis, [(i, i ^ bit) for i in range(n)])


def bits_of(n):
    return [1 << b for b in range(n.bit_length() - 1)]


def shards(projectors, wavefunctions, coupling, atom_order):
    k = 2 * projectors.shape[1]
    nkb = projectors.shape[2]
    bands = wavefunctions.shape[2]
    atoms = atom_order.shape[0]
    nh = nkb // atoms
    gr, gc = lax.axis_size("gr"), lax.axis_size("gc")
    nz, own = gr // 2, bands // gr
    local_atoms = coupling.shape[0]
    chunks = CALLS * PER_CALL
    per_block = local_atoms // chunks
    rows = per_block * nh
    me_r, me_c = lax.axis_index("gr"), lax.axis_index("gc")

    j = jnp.arange(bands, dtype=jnp.int32)
    rel_core, rel = j // (nz * own), (j // own) % nz
    rel_z = jnp.zeros_like(rel)
    for n, bit in enumerate(bits_of(nz)):
        rel_z = rel_z + bit * ((rel // (nz >> (n + 1))) % 2)
    source = (me_r ^ (2 * rel_z + rel_core)) * own + j % own
    spread = jnp.where(jnp.arange(bands, dtype=jnp.int32)[:, None] == source[None, :], 2.0, 0.0).astype(jnp.bfloat16)
    waves = jnp.dot(
        wavefunctions.reshape(k, bands), spread, preferred_element_type=jnp.float32
    ).astype(jnp.bfloat16)

    by_owner = atom_order.reshape(gc, chunks, per_block)
    owner = me_c ^ jnp.arange(gc, dtype=jnp.int32)
    listed = jnp.take(by_owner, owner, axis=0, mode="clip").transpose(1, 0, 2).reshape(CALLS, -1)

    columns = projectors.reshape(k, nkb)
    parts = []
    for call in range(CALLS):
        outs = project(columns, waves, listed[call], gc, nh, per_block)
        parts += [(outs[2 * c], outs[2 * c + 1]) for c in range(PER_CALL)]

    per_group = 8
    groups = local_atoms // per_group
    side = per_group * nh
    eye = jnp.eye(per_group, dtype=jnp.float32)
    blocks = (
        coupling.reshape(groups, per_group, nh, 1, nh) * eye[None, :, None, :, None]
    ).reshape(chunks, groups // chunks, side, side)

    pieces = []
    for c, (keep, send) in enumerate(parts):
        s = keep + swap(send, "gr", 1)
        bits = bits_of(gc)
        s = s.reshape([2] * len(bits) + [rows, s.shape[1]])
        left = bits[::-1]
        for bit in bits if c % 2 == 0 else bits[::-1]:
            axis = left.index(bit)
            left = left[:axis] + left[axis + 1:]
            mine = lax.index_in_dim(s, 0, axis, keepdims=False)
            other = lax.index_in_dim(s, 1, axis, keepdims=False)
            s = mine + swap(other, "gc", bit)
        for bit in bits_of(nz):
            half = s.shape[1] // 2
            fold = max(1, 128 // half)
            other = s[:, half:]
            if fold > 1:
                other = jnp.concatenate(jnp.split(other, fold, axis=0), axis=1)
            got = swap(other, "gr", 2 * bit)
            if fold > 1:
                got = jnp.concatenate(jnp.split(got, fold, axis=1), axis=0)
            s = s[:, :half] + got
        done = lax.dot_general(
            blocks[c], s.reshape(groups // chunks, side, s.shape[1]), (((2,), (1,)), ((0,), (0,))),
            precision=lax.Precision.HIGHEST, preferred_element_type=jnp.float32,
        )
        pieces.append(done.reshape(rows, s.shape[1]))
    return jnp.concatenate(pieces, axis=0)


def solution(mesh):
    return jax.shard_map(
        shards,
        mesh=mesh,
        in_specs=(
            P(None, ("gr", "gc"), None),
            P(None, ("gr", "gc"), None),
            P("gc", None, None),
            P(),
        ),
        out_specs=P("gc", "gr"),
        check_vma=False,
    )
```

```python
import functools

import jax
import jax.numpy as jnp
from jax import lax
from jax.experimental import pallas as pl
from jax.experimental.pallas import tpu as pltpu
from jax.sharding import PartitionSpec as P


PLAN = ((1, 1), (2, 2, 1, 1))
UNITS = 8
GROUP = 4
PAD = 8
LANES = 128


def project_body(atoms_ref, me_ref, proj_ref, waves_ref, *rest, steps, owners, nh, per_block, width, offsets, sizes, local_atoms):
    outs, nat_ref = rest[:-1], rest[-1]
    step = pl.program_id(0)
    block = proj_ref.shape[1]

    @pl.when(step < steps)
    def _():
        start = pl.multiple_of(PAD + step * block, 8)
        term = lax.dot_general(
            proj_ref[...], waves_ref[...], (((0,), (0,)), ((), ())), preferred_element_type=jnp.float32
        )
        for lane in range(term.shape[1] // LANES):
            nat_ref[lane, pl.ds(start, block), :] = term[:, lane * LANES:(lane + 1) * LANES]

    tiles = GROUP * nh // 8
    for chunk, (offset, size) in enumerate(zip(offsets, sizes)):
        keep_ref, send_ref = outs[2 * chunk], outs[2 * chunk + 1]
        first = steps + owners * sum(sizes[:chunk])

        @pl.when((step >= first) & (step < first + owners * size))
        def _():
            owner = me_ref[0] ^ ((step - first) // size)
            base = owner * local_atoms + (offset + (step - first) % size) * per_block

            @pl.loop(0, per_block // GROUP)
            def _(g):
                slot = base + g * GROUP
                starts = [atoms_ref[slot + t] * nh + PAD for t in range(GROUP)]
                for tile in range(tiles):
                    row = tile * 8
                    a = row // nh
                    at = pl.multiple_of(g * (GROUP * nh) + row, 8)
                    for lane in range(2 * width // LANES):
                        vals = nat_ref[lane, pl.ds(starts[a] + (row - a * nh), 8), :]
                        if (row + 7) // nh != a:
                            cut = (a + 1) * nh - row
                            nxt = nat_ref[lane, pl.ds(starts[a + 1] - cut, 8), :]
                            sub = lax.broadcasted_iota(jnp.int32, vals.shape, 0)
                            vals = jnp.where(sub < cut, vals, nxt)
                        out_ref = keep_ref if lane * LANES < width else send_ref
                        out_ref[pl.ds(at, 8), pl.ds(lane * LANES % width, LANES)] = vals


def project(columns, waves, atoms, me, owners, nh, per_block, offset, sizes):
    k, nkb = columns.shape
    bands = waves.shape[1]
    width = bands // 2
    block = nkb // 8
    steps = nkb // block
    rows = per_block * nh

    def out_map(first, count):
        return lambda i, *_: (jnp.clip(i - first, 0, count - 1), 0)

    specs, shapes, offsets = [], [], []
    for chunk, size in enumerate(sizes):
        offsets.append(offset + sum(sizes[:chunk]))
        for _ in range(2):
            specs.append(pl.BlockSpec((rows, width), out_map(steps + owners * sum(sizes[:chunk]), owners * size)))
            shapes.append(jax.ShapeDtypeStruct((owners * size * rows, width), jnp.float32))
    body = functools.partial(
        project_body, steps=steps, owners=owners, nh=nh, per_block=per_block, width=width,
        offsets=offsets, sizes=sizes, local_atoms=atoms.shape[0] // owners,
    )
    return pl.pallas_call(
        body,
        grid_spec=pltpu.PrefetchScalarGridSpec(
            num_scalar_prefetch=2,
            grid=(steps + owners * sum(sizes),),
            in_specs=[
                pl.BlockSpec((k, block), lambda i, *_: (0, jnp.minimum(i, steps - 1))),
                pl.BlockSpec((k, bands), lambda i, *_: (0, 0)),
            ],
            out_specs=specs,
            scratch_shapes=[pltpu.VMEM((bands // LANES, nkb + 2 * PAD, LANES), jnp.float32)],
        ),
        out_shape=shapes,
        compiler_params=pltpu.CompilerParams(
            dimension_semantics=("arbitrary",), vmem_limit_bytes=48 * 1024 * 1024
        ),
        cost_estimate=pl.CostEstimate(
            flops=2 * k * nkb * bands, transcendentals=0, bytes_accessed=2 * k * nkb + 4 * nkb * bands
        ),
    )(atoms, me, columns, waves)


def swap(x, axis, bit):
    n = lax.axis_size(axis)
    return lax.ppermute(x, axis, [(i, i ^ bit) for i in range(n)])


def bits_of(n):
    return [1 << b for b in range(n.bit_length() - 1)]


def shards(projectors, wavefunctions, coupling, atom_order):
    k = 2 * projectors.shape[1]
    nkb = projectors.shape[2]
    bands = wavefunctions.shape[2]
    atoms = atom_order.shape[0]
    nh = nkb // atoms
    gr, gc = lax.axis_size("gr"), lax.axis_size("gc")
    nz, own = gr // 2, bands // gr
    local_atoms = coupling.shape[0]
    per_block = local_atoms // UNITS
    me_r, me_c = lax.axis_index("gr"), lax.axis_index("gc")

    j = jnp.arange(bands, dtype=jnp.int32)
    rel_core, rel = j // (nz * own), (j // own) % nz
    rel_z = jnp.zeros_like(rel)
    for n, bit in enumerate(bits_of(nz)):
        rel_z = rel_z + bit * ((rel // (nz >> (n + 1))) % 2)
    source = (me_r ^ (2 * rel_z + rel_core)) * own + j % own
    spread = jnp.where(jnp.arange(bands, dtype=jnp.int32)[:, None] == source[None, :], 2.0, 0.0).astype(jnp.bfloat16)
    waves = jnp.dot(
        wavefunctions.reshape(k, bands), spread, preferred_element_type=jnp.float32
    ).astype(jnp.bfloat16)

    columns = projectors.reshape(k, nkb)
    me = me_c.astype(jnp.int32).reshape(1)
    sums, spans, offset = [], [], 0
    for sizes in PLAN:
        outs = list(project(columns, waves, atom_order, me, gc, nh, per_block, offset, sizes))
        if offset > 0:
            coupling, outs[-2] = lax.optimization_barrier((coupling, outs[-2]))
        for c, size in enumerate(sizes):
            spans.append((offset * per_block * nh, size * per_block))
            offset += size
            sums.append(outs[2 * c] + swap(outs[2 * c + 1], "gr", 1))
        if offset < UNITS:
            me, sums[-1] = lax.optimization_barrier((me, sums[-1]))

    per_group = min(8, per_block)
    side = per_group * nh
    at = jnp.arange(side, dtype=jnp.int32)
    repeat = (jnp.arange(nh, dtype=jnp.int32)[:, None] == (at % nh)[None, :]).astype(jnp.float32)
    wide = jnp.dot(coupling.reshape(local_atoms * nh, nh), repeat, precision=lax.Precision.HIGHEST)
    atom_of = (jnp.arange(local_atoms * nh, dtype=jnp.int32) // nh) % per_group
    blocks = jnp.where(atom_of[:, None] == (at // nh)[None, :], wide, 0.0)

    pieces = []
    for c, (s, (start, count)) in enumerate(zip(sums, spans)):
        rows = count * nh
        bits = bits_of(gc)
        s = s.reshape([2] * len(bits) + [rows, s.shape[1]])
        left = bits[::-1]
        for bit in bits if c % 2 == 0 else bits[::-1]:
            axis = left.index(bit)
            left = left[:axis] + left[axis + 1:]
            mine = lax.index_in_dim(s, 0, axis, keepdims=False)
            other = lax.index_in_dim(s, 1, axis, keepdims=False)
            s = mine + swap(other, "gc", bit)
        for bit in bits_of(nz):
            half = s.shape[1] // 2
            fold = max(1, LANES // half)
            other = s[:, half:]
            if fold > 1:
                other = jnp.concatenate(jnp.split(other, fold, axis=0), axis=1)
            got = swap(other, "gr", 2 * bit)
            if fold > 1:
                got = jnp.concatenate(jnp.split(got, fold, axis=1), axis=0)
            s = s[:, :half] + got
        done = lax.dot_general(
            blocks[start:start + rows].reshape(count // per_group, side, side),
            s.reshape(count // per_group, side, s.shape[1]), (((2,), (1,)), ((0,), (0,))),
            precision=lax.Precision.HIGHEST, preferred_element_type=jnp.float32,
        )
        pieces.append(done.reshape(rows, s.shape[1]))
    return jnp.concatenate(pieces, axis=0)


def solution(mesh):
    return jax.shard_map(
        shards,
        mesh=mesh,
        in_specs=(
            P(None, ("gr", "gc"), None),
            P(None, ("gr", "gc"), None),
            P("gc", None, None),
            P(),
        ),
        out_specs=P("gc", "gr"),
        check_vma=False,
    )
```

```python
import functools

import jax
import jax.numpy as jnp
from jax import lax
from jax.experimental import pallas as pl
from jax.experimental.pallas import tpu as pltpu
from jax.sharding import PartitionSpec as P


PLAN = ((1, 1), (2, 2, 1, 1))
UNITS = 8
GROUP = 4
PAD = 8
LANES = 128


def project_body(atoms_ref, me_ref, proj_ref, waves_ref, *rest, steps, owners, nh, per_block, width, offsets, sizes, local_atoms):
    outs, nat_ref = rest[:-1], rest[-1]
    step = pl.program_id(0)
    block = proj_ref.shape[1]

    @pl.when(step < steps)
    def _():
        start = pl.multiple_of(PAD + step * block, 8)
        term = lax.dot_general(
            proj_ref[...], waves_ref[...], (((0,), (0,)), ((), ())), preferred_element_type=jnp.float32
        )
        for lane in range(term.shape[1] // LANES):
            nat_ref[lane, pl.ds(start, block), :] = term[:, lane * LANES:(lane + 1) * LANES]

    tiles = GROUP * nh // 8
    for chunk, (offset, size) in enumerate(zip(offsets, sizes)):
        keep_ref, send_ref = outs[2 * chunk], outs[2 * chunk + 1]
        first = steps + owners * sum(sizes[:chunk])

        @pl.when((step >= first) & (step < first + owners * size))
        def _():
            owner = me_ref[0] ^ ((step - first) // size)
            base = owner * local_atoms + (offset + (step - first) % size) * per_block

            @pl.loop(0, per_block // GROUP)
            def _(g):
                slot = base + g * GROUP
                starts = [atoms_ref[slot + t] * nh + PAD for t in range(GROUP)]
                for tile in range(tiles):
                    row = tile * 8
                    a = row // nh
                    at = pl.multiple_of(g * (GROUP * nh) + row, 8)
                    for lane in range(2 * width // LANES):
                        vals = nat_ref[lane, pl.ds(starts[a] + (row - a * nh), 8), :]
                        if (row + 7) // nh != a:
                            cut = (a + 1) * nh - row
                            nxt = nat_ref[lane, pl.ds(starts[a + 1] - cut, 8), :]
                            sub = lax.broadcasted_iota(jnp.int32, vals.shape, 0)
                            vals = jnp.where(sub < cut, vals, nxt)
                        out_ref = keep_ref if lane * LANES < width else send_ref
                        out_ref[pl.ds(at, 8), pl.ds(lane * LANES % width, LANES)] = vals


def project(columns, waves, atoms, me, owners, nh, per_block, offset, sizes):
    k, nkb = columns.shape
    bands = waves.shape[1]
    width = bands // 2
    block = nkb // 8
    steps = nkb // block
    rows = per_block * nh

    def out_map(first, count):
        return lambda i, *_: (jnp.clip(i - first, 0, count - 1), 0)

    specs, shapes, offsets = [], [], []
    for chunk, size in enumerate(sizes):
        offsets.append(offset + sum(sizes[:chunk]))
        for _ in range(2):
            specs.append(pl.BlockSpec((rows, width), out_map(steps + owners * sum(sizes[:chunk]), owners * size)))
            shapes.append(jax.ShapeDtypeStruct((owners * size * rows, width), jnp.float32))
    body = functools.partial(
        project_body, steps=steps, owners=owners, nh=nh, per_block=per_block, width=width,
        offsets=offsets, sizes=sizes, local_atoms=atoms.shape[0] // owners,
    )
    return pl.pallas_call(
        body,
        grid_spec=pltpu.PrefetchScalarGridSpec(
            num_scalar_prefetch=2,
            grid=(steps + owners * sum(sizes),),
            in_specs=[
                pl.BlockSpec((k, block), lambda i, *_: (0, jnp.minimum(i, steps - 1))),
                pl.BlockSpec((k, bands), lambda i, *_: (0, 0)),
            ],
            out_specs=specs,
            scratch_shapes=[pltpu.VMEM((bands // LANES, nkb + 2 * PAD, LANES), jnp.float32)],
        ),
        out_shape=shapes,
        compiler_params=pltpu.CompilerParams(
            dimension_semantics=("arbitrary",), vmem_limit_bytes=48 * 1024 * 1024
        ),
        cost_estimate=pl.CostEstimate(
            flops=2 * k * nkb * bands, transcendentals=0, bytes_accessed=2 * k * nkb + 4 * nkb * bands
        ),
    )(atoms, me, columns, waves)


def swap(x, axis, bit):
    n = lax.axis_size(axis)
    return lax.ppermute(x, axis, [(i, i ^ bit) for i in range(n)])


def bits_of(n):
    return [1 << b for b in range(n.bit_length() - 1)]


def shards(projectors, wavefunctions, coupling, atom_order):
    k = 2 * projectors.shape[1]
    nkb = projectors.shape[2]
    bands = wavefunctions.shape[2]
    atoms = atom_order.shape[0]
    nh = nkb // atoms
    gr, gc = lax.axis_size("gr"), lax.axis_size("gc")
    nz, own = gr // 2, bands // gr
    local_atoms = coupling.shape[0]
    per_block = local_atoms // UNITS
    me_r, me_c = lax.axis_index("gr"), lax.axis_index("gc")

    j = jnp.arange(bands, dtype=jnp.int32)
    rel_core, rel = j // (nz * own), (j // own) % nz
    rel_z = jnp.zeros_like(rel)
    for n, bit in enumerate(bits_of(nz)):
        rel_z = rel_z + bit * ((rel // (nz >> (n + 1))) % 2)
    source = (me_r ^ (2 * rel_z + rel_core)) * own + j % own
    spread = jnp.where(jnp.arange(bands, dtype=jnp.int32)[:, None] == source[None, :], 2.0, 0.0).astype(jnp.bfloat16)
    waves = jnp.dot(
        wavefunctions.reshape(k, bands), spread, preferred_element_type=jnp.float32
    ).astype(jnp.bfloat16)

    columns = projectors.reshape(k, nkb)
    me = me_c.astype(jnp.int32).reshape(1)
    sums, spans, offset = [], [], 0
    for sizes in PLAN:
        outs = list(project(columns, waves, atom_order, me, gc, nh, per_block, offset, sizes))
        for c, size in enumerate(sizes):
            spans.append((offset * per_block * nh, size * per_block))
            offset += size
            sums.append(outs[2 * c] + swap(outs[2 * c + 1], "gr", 1))
        if offset < UNITS:
            me, sums[-1] = lax.optimization_barrier((me, sums[-1]))

    reduced = []
    for c, (s, (start, count)) in enumerate(zip(sums, spans)):
        rows = count * nh
        bits = bits_of(gc)
        s = s.reshape([2] * len(bits) + [rows, s.shape[1]])
        left = bits[::-1]
        for n, bit in enumerate(bits if c % 2 == 0 else bits[::-1]):
            axis = left.index(bit)
            left = left[:axis] + left[axis + 1:]
            mine = lax.index_in_dim(s, 0, axis, keepdims=False)
            other = lax.index_in_dim(s, 1, axis, keepdims=False)
            s = mine + swap(other, "gc", bit)
            if c == 2 and n == 0:
                coupling, s = lax.optimization_barrier((coupling, s))
        for bit in bits_of(nz):
            half = s.shape[1] // 2
            fold = max(1, LANES // half)
            other = s[:, half:]
            if fold > 1:
                other = jnp.concatenate(jnp.split(other, fold, axis=0), axis=1)
            got = swap(other, "gr", 2 * bit)
            if fold > 1:
                got = jnp.concatenate(jnp.split(got, fold, axis=1), axis=0)
            s = s[:, :half] + got
        reduced.append(s)

    per_group = min(8, per_block)
    side = per_group * nh
    at = jnp.arange(side, dtype=jnp.int32)
    repeat = (jnp.arange(nh, dtype=jnp.int32)[:, None] == (at % nh)[None, :]).astype(jnp.float32)
    wide = jnp.dot(coupling.reshape(local_atoms * nh, nh), repeat, precision=lax.Precision.HIGHEST)
    atom_of = (jnp.arange(local_atoms * nh, dtype=jnp.int32) // nh) % per_group
    blocks = jnp.where(atom_of[:, None] == (at // nh)[None, :], wide, 0.0)

    pieces = []
    for s, (start, count) in zip(reduced, spans):
        rows = count * nh
        done = lax.dot_general(
            blocks[start:start + rows].reshape(count // per_group, side, side),
            s.reshape(count // per_group, side, s.shape[1]), (((2,), (1,)), ((0,), (0,))),
            precision=lax.Precision.HIGHEST, preferred_element_type=jnp.float32,
        )
        pieces.append(done.reshape(rows, s.shape[1]))
    return jnp.concatenate(pieces, axis=0)


def solution(mesh):
    return jax.shard_map(
        shards,
        mesh=mesh,
        in_specs=(
            P(None, ("gr", "gc"), None),
            P(None, ("gr", "gc"), None),
            P("gc", None, None),
            P(),
        ),
        out_specs=P("gc", "gr"),
        check_vma=False,
    )
```
